32 devices in a mesh: shot: 4 (over y, core), space: 8 (over z, x).
Axes of the slice: x: 2, y: 2, z: 4, core: 2. Of those that a mesh axis runs over, the one named last changes fastest.
Arguments:
- adjoint_now: float32 [4, 128, 64, 512], P('shot', 'space'), may hold values from -6 to 6
- adjoint_later: float32 [4, 128, 64, 512], P('shot', 'space'), may hold values from -6 to 6
- courant: float32 [128, 64, 512], P('space'), may hold values from 0.05 to 0.2
- checkpoint_codes: int32 [4, 6, 128, 64, 128], P('shot', None, 'space'), may hold values from -2147483648 to 2147483646
- scale_index: int32 [4, 6, 128, 256], P('shot', None, 'space'), may hold values from 0 to 63
- scale_table: float32 [64], replicated, may hold values from 0.001 to 0.01
- receiver_cell: int32 [4, 2048], P('shot', 'space'), may hold values from 0 to 4194303, as said below
- observed: float32 [4, 4, 2048], P('shot', None, 'space'), may hold values from -12 to 12
- source_cell: int32 [4, 3], P('shot'), may hold values from 0 to 511, as said below
Outputs:
- gradient: float32 [128, 64, 512], P('space', 'shot')
- adjoint_first: float32 [4, 128, 64, 512], P('shot', 'space')
- adjoint_second: float32 [4, 128, 64, 512], P('shot', 'space')
- misfit: float32 [], replicated
The draws below stay inside these ranges and needn't reach their ends.
Inputs may be any that keep to these rules, and one draw needn't show every extreme that they name: `receiver_cell`: for every r, entries r * 256 to (r + 1) * 256 - 1 of each shot's row are flat indices (z * 64 + y) * 512 + x of cells with r * 16 <= z < (r + 1) * 16. `source_cell`: column 0 is a z index below 128, column 1 a y index below 64, column 2 an x index below 512.
All inputs are finite; a program needn't handle non-finite values.
Results may differ from the reference program's by a relative error of at most 0.0001.
Values sent between devices are 32-bit elements; how exact they have to be, the bound alone decides.
A program may use at most 128 MiB of HBM per device.

```python
import math
import jax
import jax.numpy as jnp

NX = 512
NY = 64
CZ = 16
ITERS = 4
QBLOCK = 128
SCALES = 64
MUTE = 8
REC_DEV = 256
LEVELS = 6
NZ = 128
SHOTS = 4
RECEIVERS = 2048


def draw_receiver_cell(key, part):
    keys = jax.random.split(jax.random.fold_in(key, 11), 3)
    slab = jnp.arange(RECEIVERS, dtype=jnp.int32) // REC_DEV
    depth = slab * CZ + jax.random.randint(keys[0], (SHOTS, RECEIVERS), 0, CZ)
    row = jax.random.randint(keys[1], (SHOTS, RECEIVERS), 0, NY)
    col = jax.random.randint(keys[2], (SHOTS, RECEIVERS), 0, NX)
    return ((depth * NY + row) * NX + col).astype(jnp.int32)


def draw_observed(key, part):
    ramp = 1.0 + 2.0 * jnp.arange(RECEIVERS, dtype=jnp.float32) / RECEIVERS
    base = jnp.clip(jax.random.normal(jax.random.fold_in(key, 22), (SHOTS, ITERS, RECEIVERS), jnp.float32), -4.0, 4.0)
    return (base * ramp).astype(jnp.float32)


def draw_source_cell(key, part):
    keys = jax.random.split(jax.random.fold_in(key, 31), 4)
    depth = jax.random.randint(keys[0], (SHOTS, 1), 0, NZ)
    row = jax.random.randint(keys[1], (SHOTS, 1), 0, NY)
    col = jax.random.randint(keys[2], (SHOTS, 1), 0, NX)
    chosen = jax.random.randint(keys[3], (), 0, SHOTS)
    marked = (jnp.arange(SHOTS, dtype=jnp.int32) == chosen).reshape(SHOTS, 1)
    depth = jnp.where(marked, NZ - 1, depth)
    row = jnp.where(marked, 0, row)
    return jnp.concatenate([depth, row, col], axis=1).astype(jnp.int32)


def set_ends(entries, key, smallest, largest):
    index_at = [jax.random.randint(jax.random.fold_in(key, axis), (), 0, length) for axis, length in enumerate(entries.shape)]
    longest = entries.shape.index(max(entries.shape))
    neighbour = index_at[:longest] + [(index_at[longest] + 1) % entries.shape[longest]] + index_at[longest + 1:]
    return entries.at[tuple(index_at)].set(smallest).at[tuple(neighbour)].set(largest)


def block_scale(rng, dims, cuts, low, high):
    loudness = 1.0
    for dim, parts in cuts:
        draws = jax.random.uniform(jax.random.fold_in(jax.random.fold_in(rng, 6), dim), (parts,), jnp.float32, low / len(cuts), high / len(cuts))
        loudness = loudness * jnp.repeat(jnp.exp(draws), dims[dim] // parts).reshape((-1,) + (1,) * (len(dims) - 1 - dim))
    return loudness


def scatter_about(key, shape, width, limit, shards=(), kind=jnp.bfloat16):
    gain = block_scale(key, shape, shards, -0.22, 0.18) if shards else 1.0
    values = jax.random.normal(key, shape, jnp.float32) * width * gain
    return jnp.minimum(jnp.maximum(values, -limit), limit).astype(kind)


def setup_inputs(seed: int = 0) -> dict:
    seeds = jax.random.split(jax.random.key(seed), 10)
    return {
        "adjoint_now": scatter_about(seeds[0], (SHOTS, NZ, NY, NX), 1.0, 6.0, ((0, 4), (1, 8)), jnp.float32),
        "adjoint_later": scatter_about(seeds[1], (SHOTS, NZ, NY, NX), 1.0, 6.0, ((0, 4), (1, 8)), jnp.float32),
        "courant": jnp.clip(jnp.exp(math.log(0.2) - 1.3862944 * jax.random.uniform(seeds[2], (NZ, NY, NX), jnp.float32) ** block_scale(seeds[2], (NZ, NY, NX), ((0, 8),), -0.2, 0.2)), 0.05, 0.2),
        "checkpoint_codes": set_ends(jax.random.randint(seeds[3], (SHOTS, LEVELS, NZ, NY, NX // 4), -2147483648, 2147483647), jax.random.fold_in(seeds[3], 1), -2147483648, 2147483646).astype(jnp.int32),
        "scale_index": set_ends(jax.random.randint(seeds[4], (SHOTS, LEVELS, NZ, NY * NX // QBLOCK), 0, SCALES), jax.random.fold_in(seeds[4], 1), 0, SCALES - 1).astype(jnp.int32),
        "scale_table": jnp.clip(jnp.exp(jax.random.uniform(seeds[5], (SCALES,), jnp.float32, math.log(0.001), math.log(0.01))), 0.001, 0.01),
        "receiver_cell": draw_receiver_cell(jax.random.fold_in(seeds[9], 71), 0),
        "observed": draw_observed(jax.random.fold_in(seeds[9], 71), 0),
        "source_cell": draw_source_cell(jax.random.fold_in(seeds[9], 71), 0),
    }


COEFFS = (-205.0 / 72.0, 8.0 / 5.0, -1.0 / 5.0, 8.0 / 315.0, -1.0 / 560.0)


def decode(words, index, table):
    planes = [jnp.bitwise_and(jnp.right_shift(words, 8 * m), 255) for m in range(4)]
    codes = jnp.concatenate(planes, axis=-1)
    centred = (codes - 128).astype(jnp.float32)
    depth, rows, cols = centred.shape
    scale = table[index]
    blocks = centred.reshape(depth, rows, cols // QBLOCK, QBLOCK) * scale.reshape(depth, rows, cols // QBLOCK, 1)
    return blocks.reshape(depth, rows, cols)


def laplace(field):
    padded = jnp.pad(field, 4)
    depth, rows, cols = field.shape
    total = 3.0 * COEFFS[0] * field
    for step in range(1, 5):
        total = total + COEFFS[step] * (padded[4 + step:4 + step + depth, 4:4 + rows, 4:4 + cols] + padded[4 - step:4 - step + depth, 4:4 + rows, 4:4 + cols])
        total = total + COEFFS[step] * (padded[4:4 + depth, 4 + step:4 + step + rows, 4:4 + cols] + padded[4:4 + depth, 4 - step:4 - step + rows, 4:4 + cols])
        total = total + COEFFS[step] * (padded[4:4 + depth, 4:4 + rows, 4 + step:4 + step + cols] + padded[4:4 + depth, 4:4 + rows, 4 - step:4 - step + cols])
    return total


def reference(adjoint_now, adjoint_later, courant, checkpoint_codes, scale_index, scale_table, receiver_cell, observed, source_cell):
    gradient = jnp.zeros((NZ, NY, NX), jnp.float32)
    misfit_sum = jnp.zeros((), jnp.float32)
    firsts = []
    seconds = []
    zpos = jnp.arange(NZ, dtype=jnp.int32).reshape(NZ, 1, 1)
    ypos = jnp.arange(NY, dtype=jnp.int32).reshape(1, NY, 1)
    xpos = jnp.arange(NX, dtype=jnp.int32).reshape(1, 1, NX)
    for shot in range(SHOTS):
        fields = [decode(checkpoint_codes[shot, level], scale_index[shot, level], scale_table) for level in range(ITERS + 2)]
        now = adjoint_now[shot]
        later = adjoint_later[shot]
        image = jnp.zeros((NZ, NY, NX), jnp.float32)
        cells = receiver_cell[shot]
        for step in range(ITERS):
            level = ITERS - step
            synthetic = jnp.take(fields[level].reshape(-1), cells)
            residual = synthetic - observed[shot, level - 1]
            misfit_sum = misfit_sum + jnp.sum(residual * residual)
            image = image + now * (fields[level + 1] - 2.0 * fields[level] + fields[level - 1])
            stepped = 2.0 * now - later + courant * laplace(now)
            stepped = stepped.reshape(-1).at[cells].add(residual).reshape(NZ, NY, NX)
            later = now
            now = stepped
        source = source_cell[shot]
        dist = ((zpos - source[0]) ** 2 + (ypos - source[1]) ** 2 + (xpos - source[2]) ** 2).astype(jnp.float32)
        mute = 1.0 - jnp.exp(-dist / (2.0 * MUTE * MUTE))
        gradient = gradient + image * mute
        firsts.append(now)
        seconds.append(later)
    misfit = 0.5 * misfit_sum / (SHOTS * ITERS * RECEIVERS)
    return gradient, jnp.stack(firsts), jnp.stack(seconds), misfit
```

```python
import functools

import jax
import jax.numpy as jnp
from jax import lax
from jax.experimental import pallas as pl
from jax.experimental.pallas import tpu as pltpu
from jax.sharding import PartitionSpec as P

ITERS = 4
QBLOCK = 128
MUTE = 8
W = 4
NC = 2
F32 = jnp.float32
BF16 = jnp.bfloat16
MESH = pl.DeviceIdType.MESH

COEFFS = (-205.0 / 72.0, 8.0 / 5.0, -1.0 / 5.0, 8.0 / 315.0, -1.0 / 560.0)


def split(value):
    high = value.astype(BF16)
    return high, (value - high.astype(F32)).astype(BF16)


def dot(a, b):
    return jnp.dot(a, b, preferred_element_type=F32)


def band(rows, cols, first):
    i = first + lax.broadcasted_iota(jnp.int32, (rows, cols), 0)
    j = lax.broadcasted_iota(jnp.int32, (rows, cols), 1)
    d = jnp.abs(i - j)
    value = jnp.zeros((rows, cols), F32)
    for k in range(1, 5):
        value = jnp.where(d == k, COEFFS[k], value)
    return split(value)


def kernel(
    nshot,
    nspace,
    cells_s,
    source_s,
    table,
    now_h,
    later_h,
    cour,
    words,
    index,
    cells_row,
    cells_col,
    observed,
    grad,
    first_h,
    second_h,
    misfit,
    E,
    D,
    scales,
    IM,
    RA,
    S,
    RB,
    PR,
    QH,
    QL,
    CH,
    CL,
    GW,
    GS,
    MB,
    SB,
    MT,
    ST,
    halo_send,
    halo_recv,
    a_send,
    a_recv,
    b_send,
    b_recv,
    m_send,
    m_recv,
    s_send,
    s_recv,
    local_sem,
):
    depth, rows, cols = cour.shape
    nrec = cells_col.shape[0]
    ych = rows // NC
    shot = lax.axis_index("shot")
    space = lax.axis_index("space")
    has_low = space > 0
    has_high = space < nspace - 1

    barrier = pltpu.get_barrier_semaphore()
    for d in range(1, nshot):
        pl.semaphore_signal(
            barrier, inc=1, device_id={"shot": lax.rem(shot + d, nshot)}, device_id_type=MESH
        )

    @pl.loop(1, nspace)
    def _(d):
        pl.semaphore_signal(
            barrier, inc=1, device_id={"space": lax.rem(space + d, nspace)}, device_id_type=MESH
        )

    pl.semaphore_wait(barrier, nshot + nspace - 2)

    def halo(t, c, up):
        ys = pl.ds(c * ych, ych)
        src_z = W + depth - W if up else W
        dst_z = 0 if up else W + depth
        return pltpu.make_async_remote_copy(
            src_ref=E.at[t + 1, pl.ds(src_z, W), ys, :],
            dst_ref=E.at[t + 1, pl.ds(dst_z, W), ys, :],
            send_sem=halo_send.at[int(up), t, c],
            recv_sem=halo_recv.at[int(up), t, c],
            device_id={"space": space + (1 if up else -1)},
            device_id_type=MESH,
        )

    def halo_first(c, up):
        ys = pl.ds(c * ych, ych)
        src_z = depth - W if up else 0
        dst_z = 0 if up else W + depth
        return pltpu.make_async_remote_copy(
            src_ref=now_h.at[pl.ds(src_z, W), ys, :],
            dst_ref=E.at[1, pl.ds(dst_z, W), ys, :],
            send_sem=halo_send.at[int(up), 0, c],
            recv_sem=halo_recv.at[int(up), 0, c],
            device_id={"space": space + (1 if up else -1)},
            device_id_type=MESH,
        )

    for c in range(NC):

        @pl.when(has_high)
        def _():
            halo_first(c, True).start()

        @pl.when(has_low)
        def _():
            halo_first(c, False).start()

    in_now = pltpu.make_async_copy(now_h, E.at[1, pl.ds(W, depth)], local_sem.at[0])
    in_later = pltpu.make_async_copy(later_h, E.at[0, pl.ds(W, depth)], local_sem.at[1])
    in_now.start()
    in_later.start()

    @pl.loop(0, cols // 64)
    def _(i):
        start = pl.multiple_of(i * 64, 64)
        high, low = band(64, cols, start)
        CH[pl.ds(start, 64), :] = high
        CL[pl.ds(start, 64), :] = low

    yh, yl = band(rows, rows, 0)

    @pl.loop(0, depth)
    def _(z):
        entry = index[z]
        scale = jnp.zeros(entry.shape, F32)
        for e in range(table.shape[0]):
            scale = jnp.where(entry == e, table[e], scale)
        scales[z] = scale

    slab = depth * rows * cols

    @pl.loop(0, nrec)
    def _(r):
        cell = lax.rem(cells_s[r], slab)
        row = cell // cols
        z = row // rows
        y = lax.rem(row, rows)
        for k in range(1, ITERS + 1):
            GW[k - 1, pl.ds(r, 1), :] = words[k, z, pl.ds(y, 1), :]
        GS[pl.ds(r, 1), :] = scales[z, pl.ds(y, 1), :]

    xcol = lax.rem(cells_col[...], cols)
    mcol = xcol // QBLOCK
    jcol = lax.rem(xcol, QBLOCK)
    lane = lax.broadcasted_iota(jnp.int32, (nrec, QBLOCK), 1)
    xl = lax.broadcasted_iota(jnp.int32, (nrec, cols), 1)
    squares = jnp.zeros((1, 1), F32)
    for k in range(1, ITERS + 1):
        code = jnp.bitwise_and(jnp.right_shift(GW[k - 1], 8 * mcol), 255) - 128
        code = jnp.sum(jnp.where(lane == jcol, code.astype(F32), 0.0), axis=1, keepdims=True)
        scale = jnp.sum(
            jnp.where(lane == k * 4 + mcol, GS[...], 0.0), axis=1, keepdims=True
        )
        residual = code * scale - observed[:, k - 1 : k]
        squares = squares + jnp.sum(residual * residual, axis=0, keepdims=True)
        high, low = split(jnp.where(xl == xcol, residual, 0.0))
        QH[ITERS - k] = high
        QL[ITERS - k] = low
    crow = lax.rem(cells_row[...], slab) // cols
    for z in range(depth):
        i = z * rows + lax.broadcasted_iota(jnp.int32, (rows, nrec), 0)
        PR[z] = jnp.where(i == crow, 1.0, 0.0).astype(BF16)

    tile = jnp.broadcast_to(squares, (8, 128))
    MT[...] = tile
    MB[pl.ds(shot, 1)] = tile.reshape(1, 8, 128)

    def misfit_copy(d):
        return pltpu.make_async_remote_copy(
            src_ref=MT,
            dst_ref=MB.at[shot],
            send_sem=m_send.at[d - 1],
            recv_sem=m_recv.at[d - 1],
            device_id={"shot": lax.rem(shot + d, nshot)},
            device_id_type=MESH,
        )

    def total_copy(d):
        return pltpu.make_async_remote_copy(
            src_ref=ST,
            dst_ref=SB.at[space],
            send_sem=s_send.at[d - 1],
            recv_sem=s_recv.at[d - 1],
            device_id={"space": lax.rem(space + d, nspace)},
            device_id_type=MESH,
        )

    for d in range(1, nshot):
        misfit_copy(d).start()

    in_now.wait()
    in_later.wait()

    def local(t):
        for g in (0, depth // W - 1) + tuple(range(1, depth // W - 1)):
            z0 = g * W
            u = E[t + 1, W + z0 : W + z0 + W].reshape(W * rows, cols)
            uh, ul = split(u)
            lap = dot(uh, CH[...]) + dot(ul, CH[...]) + dot(uh, CL[...])
            for j in range(W):
                z = z0 + j
                part = slice(j * rows, (j + 1) * rows)
                up = u[part]
                acc = lap[part] + (3.0 * COEFFS[0]) * up
                acc = acc + dot(yh, uh[part]) + dot(yh, ul[part]) + dot(yl, uh[part])
                for i in range(1, 5):
                    if z + i < depth:
                        acc = acc + COEFFS[i] * E[t + 1, W + z + i]
                    if z - i >= 0:
                        acc = acc + COEFFS[i] * E[t + 1, W + z - i]
                inject = dot(PR[z], QH[t]) + dot(PR[z], QL[t])
                E[t + 2, W + z] = 2.0 * up - E[t, W + z] + cour[z] * acc + inject

    local(0)

    @pl.loop(0, depth)
    def _(z):
        for m in range(cols // QBLOCK):
            xs = slice(m * QBLOCK, (m + 1) * QBLOCK)
            f = []
            for k in range(ITERS + 2):
                code = jnp.bitwise_and(jnp.right_shift(words[k, z], 8 * m), 255) - 128
                f.append(code.astype(F32) * scales[z, :, k * 4 + m : k * 4 + m + 1])
            for t in range(ITERS):
                k = ITERS - t
                diff = f[k + 1] - 2.0 * f[k] + f[k - 1]
                if t == 0:
                    IM[z, :, xs] = E[1, W + z, :, xs] * diff
                else:
                    D[t - 1, z, :, xs] = diff

    for d in range(1, nshot):
        misfit_copy(d).wait()
    total = MB[0]
    for d in range(1, nshot):
        total = total + MB[d]
    ST[...] = total
    SB[pl.ds(space, 1)] = total.reshape(1, 8, 128)

    @pl.loop(1, nspace)
    def _(d):
        total_copy(d).start()

    def fix(t, c):
        ys = pl.ds(c * ych, ych)

        @pl.when(has_low)
        def _():
            halo(t, c, True).wait_recv()
            for j in range(W):
                acc = COEFFS[j + 1] * E[t + 1, W - 1, ys, :]
                for i in range(j + 2, 5):
                    acc = acc + COEFFS[i] * E[t + 1, W + j - i, ys, :]
                E[t + 2, W + j, ys, :] += cour[j, ys, :] * acc

        @pl.when(has_high)
        def _():
            halo(t, c, False).wait_recv()
            for j in range(W):
                z = depth - 1 - j
                acc = COEFFS[j + 1] * E[t + 1, W + depth, ys, :]
                for i in range(j + 2, 5):
                    acc = acc + COEFFS[i] * E[t + 1, W + z + i, ys, :]
                E[t + 2, W + z, ys, :] += cour[z, ys, :] * acc

    @pl.loop(0, ITERS - 1)
    def _(t):
        for c in range(NC):
            fix(t, c)

            @pl.when(has_high)
            def _():
                halo(t + 1, c, True).start()

            @pl.when(has_low)
            def _():
                halo(t + 1, c, False).start()

        local(t + 1)

        @pl.loop(0, depth)
        def _(z):
            IM[z] = IM[z] + E[t + 2, W + z] * D[t, z]

    out_second = pltpu.make_async_copy(E.at[ITERS, pl.ds(W, depth)], second_h, local_sem.at[2])
    out_second.start()

    first_z = space * depth

    @pl.loop(0, depth)
    def _(z):
        dz = first_z + z - source_s[0]
        dy = lax.broadcasted_iota(jnp.int32, (rows, cols), 0) - source_s[1]
        dx = lax.broadcasted_iota(jnp.int32, (rows, cols), 1) - source_s[2]
        dist = (dz * dz + dy * dy + dx * dx).astype(F32)
        IM[z] = IM[z] * (1.0 - jnp.exp(dist * (-1.0 / (2.0 * MUTE * MUTE))))

    core = lax.rem(shot, 2)
    pair = shot // 2
    pairs = nshot // 2
    yq = rows // nshot

    def quarter(index):
        return pl.ds(pl.multiple_of(index * yq, yq), yq)

    def copy_a(h):
        return pltpu.make_async_remote_copy(
            src_ref=IM.at[:, quarter(2 * h + 1 - core), :],
            dst_ref=RA.at[h],
            send_sem=a_send.at[h],
            recv_sem=a_recv.at[h],
            device_id={"shot": shot + 1 - 2 * core},
            device_id_type=MESH,
        )

    def copy_b(d):
        target = lax.rem(pair + d, pairs)
        return pltpu.make_async_remote_copy(
            src_ref=S.at[target],
            dst_ref=RB.at[d - 1],
            send_sem=b_send.at[d - 1],
            recv_sem=b_recv.at[d - 1],
            device_id={"shot": 2 * target + core},
            device_id_type=MESH,
        )

    for h in range(pairs):
        copy_a(h).start()
    for h in range(pairs):
        copy_a(h).wait()
        S[h] = IM[:, quarter(2 * h + core), :] + RA[h]
    for d in range(1, pairs):
        copy_b(d).start()

    for c in range(NC):
        fix(ITERS - 1, c)
    out_first = pltpu.make_async_copy(E.at[ITERS + 1, pl.ds(W, depth)], first_h, local_sem.at[3])
    out_first.start()

    total = S[pair]
    for d in range(1, pairs):
        copy_b(d).wait()
        total = total + RB[d - 1]
    grad[...] = total

    @pl.loop(1, nspace)
    def _(d):
        total_copy(d).wait()

    whole = SB[0]
    for d in range(1, nspace):
        whole = whole + SB[d]
    misfit[...] = whole

    for c in range(NC):

        @pl.when(has_high)
        def _():
            halo_first(c, True).wait_send()

        @pl.when(has_low)
        def _():
            halo_first(c, False).wait_send()

        @pl.loop(1, ITERS)
        def _(t):
            @pl.when(has_high)
            def _():
                halo(t, c, True).wait_send()

            @pl.when(has_low)
            def _():
                halo(t, c, False).wait_send()

    out_second.wait()
    out_first.wait()


def body(
    nshot,
    nspace,
    adjoint_now,
    adjoint_later,
    courant,
    checkpoint_codes,
    scale_index,
    scale_table,
    receiver_cell,
    observed,
    source_cell,
):
    depth, rows, cols = courant.shape
    levels = checkpoint_codes.shape[1]
    nrec = receiver_cell.shape[1]
    blocks = cols // QBLOCK
    index = scale_index[0].reshape(levels, depth, rows, blocks).transpose(1, 2, 0, 3)
    index = index.reshape(depth, rows, levels * blocks)
    index = jnp.pad(index, ((0, 0), (0, 0), (0, 128 - levels * blocks)))
    pairs = nshot // 2
    yq = rows // nshot
    vmem = pl.BlockSpec(memory_space=pltpu.VMEM)
    smem = pl.BlockSpec(memory_space=pltpu.SMEM)
    anyspace = pl.BlockSpec(memory_space=pl.ANY)
    dma = pltpu.SemaphoreType.DMA
    field = jax.ShapeDtypeStruct((depth, rows, cols), F32)
    gradient, first, second, misfit = pl.pallas_call(
        functools.partial(kernel, nshot, nspace),
        out_shape=(
            jax.ShapeDtypeStruct((depth, yq, cols), F32),
            field,
            field,
            jax.ShapeDtypeStruct((8, 128), F32),
        ),
        in_specs=[smem, smem, smem, anyspace, anyspace] + [vmem] * 6,
        out_specs=(vmem, anyspace, anyspace, vmem),
        scratch_shapes=[
            pltpu.VMEM((ITERS + 2, depth + 2 * W, rows, cols), F32),
            pltpu.VMEM((ITERS - 1, depth, rows, cols), F32),
            pltpu.VMEM((depth, rows, 128), F32),
            pltpu.VMEM((depth, rows, cols), F32),
            pltpu.VMEM((pairs, depth, yq, cols), F32),
            pltpu.VMEM((pairs, depth, yq, cols), F32),
            pltpu.VMEM((max(pairs - 1, 1), depth, yq, cols), F32),
            pltpu.VMEM((depth, rows, nrec), BF16),
            pltpu.VMEM((ITERS, nrec, cols), BF16),
            pltpu.VMEM((ITERS, nrec, cols), BF16),
            pltpu.VMEM((cols, cols), BF16),
            pltpu.VMEM((cols, cols), BF16),
            pltpu.VMEM((ITERS, nrec, QBLOCK), jnp.int32),
            pltpu.VMEM((nrec, 128), F32),
            pltpu.VMEM((nshot, 8, 128), F32),
            pltpu.VMEM((nspace, 8, 128), F32),
            pltpu.VMEM((8, 128), F32),
            pltpu.VMEM((8, 128), F32),
            dma((2, ITERS, NC)),
            dma((2, ITERS, NC)),
            dma((pairs,)),
            dma((pairs,)),
            dma((max(pairs - 1, 1),)),
            dma((max(pairs - 1, 1),)),
            dma((nshot - 1,)),
            dma((nshot - 1,)),
            dma((nspace - 1,)),
            dma((nspace - 1,)),
            dma((4,)),
        ],
        compiler_params=pltpu.CompilerParams(
            collective_id=0, has_side_effects=True, vmem_limit_bytes=66000000
        ),
    )(
        receiver_cell[0],
        source_cell[0],
        scale_table,
        adjoint_now[0],
        adjoint_later[0],
        courant,
        checkpoint_codes[0],
        index,
        receiver_cell,
        receiver_cell.reshape(nrec, 1),
        observed[0].T,
    )
    count = nshot * ITERS * nrec * nspace
    return (gradient, first[None], second[None], 0.5 * misfit[0, 0] / count)


def solution(mesh):
    placed = (
        P("shot", "space", None, None),
        P("shot", "space", None, None),
        P("space", None, None),
        P("shot", None, "space", None, None),
        P("shot", None, "space", None),
        P(),
        P("shot", "space"),
        P("shot", None, "space"),
        P("shot", None),
    )
    return jax.shard_map(
        functools.partial(body, mesh.shape["shot"], mesh.shape["space"]),
        mesh=mesh,
        in_specs=placed,
        out_specs=(
            P("space", "shot", None),
            P("shot", "space", None, None),
            P("shot", "space", None, None),
            P(),
        ),
        check_vma=False,
    )
```

```python
import functools

import jax
import jax.numpy as jnp
from jax import lax
from jax.experimental import pallas as pl
from jax.experimental.pallas import tpu as pltpu
from jax.sharding import PartitionSpec as P

ITERS = 4
QBLOCK = 128
MUTE = 8
W = 4
NC = 2
F32 = jnp.float32
BF16 = jnp.bfloat16
MESH = pl.DeviceIdType.MESH

COEFFS = (-205.0 / 72.0, 8.0 / 5.0, -1.0 / 5.0, 8.0 / 315.0, -1.0 / 560.0)


def split(value):
    high = value.astype(BF16)
    return high, (value - high.astype(F32)).astype(BF16)


def dot(a, b):
    return jnp.dot(a, b, preferred_element_type=F32)


def band(rows, cols, first):
    i = first + lax.broadcasted_iota(jnp.int32, (rows, cols), 0)
    j = lax.broadcasted_iota(jnp.int32, (rows, cols), 1)
    d = jnp.abs(i - j)
    value = jnp.zeros((rows, cols), F32)
    for k in range(1, 5):
        value = jnp.where(d == k, COEFFS[k], value)
    return split(value)


def kernel(
    nshot,
    nspace,
    cells_s,
    source_s,
    table,
    observed,
    now_h,
    later_h,
    cour_h,
    words_h,
    index,
    cells_row,
    grad,
    first_h,
    second_h,
    misfit,
    E,
    D,
    cour,
    words,
    SC,
    TS,
    PC,
    OB,
    IM,
    RA,
    S,
    RB,
    PR,
    QH,
    QL,
    CH,
    CL,
    GW,
    GS,
    MB,
    SB,
    MT,
    ST,
    halo_send,
    halo_recv,
    a_send,
    a_recv,
    b_send,
    b_recv,
    m_send,
    m_recv,
    s_send,
    s_recv,
    local_sem,
):
    depth, rows, cols = cour.shape
    nrec = cells_row.shape[1]
    blocks = cols // QBLOCK
    ych = rows // NC
    shot = lax.axis_index("shot")
    space = lax.axis_index("space")
    has_low = space > 0
    has_high = space < nspace - 1

    barrier = pltpu.get_barrier_semaphore()
    for d in range(1, nshot):
        pl.semaphore_signal(
            barrier, inc=1, device_id={"shot": lax.rem(shot + d, nshot)}, device_id_type=MESH
        )

    @pl.loop(1, nspace)
    def _(d):
        pl.semaphore_signal(
            barrier, inc=1, device_id={"space": lax.rem(space + d, nspace)}, device_id_type=MESH
        )

    in_now = pltpu.make_async_copy(now_h, E.at[1, pl.ds(W, depth)], local_sem.at[0])
    in_later = pltpu.make_async_copy(later_h, E.at[0, pl.ds(W, depth)], local_sem.at[1])
    in_cour = pltpu.make_async_copy(cour_h, cour, local_sem.at[2])
    in_words = pltpu.make_async_copy(words_h, words, local_sem.at[3])
    in_words.start()
    in_now.start()
    in_cour.start()
    in_later.start()

    pl.semaphore_wait(barrier, nshot + nspace - 2)

    def halo(t, c, up):
        ys = pl.ds(c * ych, ych)
        src_z = W + depth - W if up else W
        dst_z = 0 if up else W + depth
        return pltpu.make_async_remote_copy(
            src_ref=E.at[t + 1, pl.ds(src_z, W), ys, :],
            dst_ref=E.at[t + 1, pl.ds(dst_z, W), ys, :],
            send_sem=halo_send.at[int(up), t, c],
            recv_sem=halo_recv.at[int(up), t, c],
            device_id={"space": space + (1 if up else -1)},
            device_id_type=MESH,
        )

    def halo_first(c, up):
        ys = pl.ds(c * ych, ych)
        src_z = depth - W if up else 0
        dst_z = 0 if up else W + depth
        return pltpu.make_async_remote_copy(
            src_ref=now_h.at[pl.ds(src_z, W), ys, :],
            dst_ref=E.at[1, pl.ds(dst_z, W), ys, :],
            send_sem=halo_send.at[int(up), 0, c],
            recv_sem=halo_recv.at[int(up), 0, c],
            device_id={"space": space + (1 if up else -1)},
            device_id_type=MESH,
        )

    for c in range(NC):

        @pl.when(has_high)
        def _():
            halo_first(c, True).start()

        @pl.when(has_low)
        def _():
            halo_first(c, False).start()

    @pl.loop(0, cols // 64)
    def _(i):
        start = pl.multiple_of(i * 64, 64)
        high, low = band(64, cols, start)
        CH[pl.ds(start, 64), :] = high
        CL[pl.ds(start, 64), :] = low

    yh, yl = band(rows, rows, 0)

    entry = index[...]
    scale = jnp.zeros(entry.shape, F32)
    for e in range(table.shape[0]):
        scale = jnp.where(entry == e, table[e], scale)
    levels = entry.shape[0]
    SC[0:levels] = scale
    SC[levels:] = jnp.zeros((SC.shape[0] - levels,) + entry.shape[1:], F32)

    slab = depth * rows * cols
    in_words.wait()

    @pl.loop(0, nrec, unroll=4)
    def _(r):
        cell = lax.rem(cells_s[r], slab)
        row = cell // cols
        z = row // rows
        y = lax.rem(row, rows)
        for k in range(1, ITERS + 1):
            GW[k - 1, pl.ds(r, 1), :] = words[k, z, pl.ds(y, 1), :]
            GS[k - 1, pl.ds(r, 1), :] = SC[k, pl.ds(z, 1), :]
            OB[k - 1, pl.ds(r, 1), :] = jnp.full((1, 128), observed[k - 1, r], F32)
        PC[pl.ds(r, 1), :] = jnp.full((1, 128), cell - z * (rows * cols), jnp.int32)

    place = PC[:, 0:1]
    xcol = lax.rem(place, cols)
    mcol = xcol // QBLOCK
    jcol = lax.rem(xcol, QBLOCK)
    scol = place // cols * blocks + mcol
    lane = lax.broadcasted_iota(jnp.int32, (nrec, QBLOCK), 1)
    sl = lax.broadcasted_iota(jnp.int32, (nrec, rows * blocks), 1)
    xl = lax.broadcasted_iota(jnp.int32, (nrec, cols), 1)
    squares = jnp.zeros((1, 1), F32)
    for k in range(1, ITERS + 1):
        code = jnp.bitwise_and(jnp.right_shift(GW[k - 1], 8 * mcol), 255) - 128
        code = jnp.sum(jnp.where(lane == jcol, code.astype(F32), 0.0), axis=1, keepdims=True)
        scale = jnp.sum(jnp.where(sl == scol, GS[k - 1], 0.0), axis=1, keepdims=True)
        residual = code * scale - OB[k - 1, :, 0:1]
        squares = squares + jnp.sum(residual * residual, axis=0, keepdims=True)
        high, low = split(jnp.where(xl == xcol, residual, 0.0))
        QH[ITERS - k] = high
        QL[ITERS - k] = low
    crow = lax.rem(cells_row[...], slab) // cols
    for z in range(depth):
        i = z * rows + lax.broadcasted_iota(jnp.int32, (rows, nrec), 0)
        PR[z] = jnp.where(i == crow, 1.0, 0.0).astype(BF16)

    tile = jnp.broadcast_to(squares, (8, 128))
    MT[...] = tile
    MB[pl.ds(shot, 1)] = tile.reshape(1, 8, 128)

    def misfit_copy(d):
        return pltpu.make_async_remote_copy(
            src_ref=MT,
            dst_ref=MB.at[shot],
            send_sem=m_send.at[d - 1],
            recv_sem=m_recv.at[d - 1],
            device_id={"shot": lax.rem(shot + d, nshot)},
            device_id_type=MESH,
        )

    def total_copy(d):
        return pltpu.make_async_remote_copy(
            src_ref=ST,
            dst_ref=SB.at[space],
            send_sem=s_send.at[d - 1],
            recv_sem=s_recv.at[d - 1],
            device_id={"space": lax.rem(space + d, nspace)},
            device_id_type=MESH,
        )

    for d in range(1, nshot):
        misfit_copy(d).start()

    in_now.wait()
    in_later.wait()
    in_cour.wait()

    def local(t):
        for g in (0, depth // W - 1) + tuple(range(1, depth // W - 1)):
            z0 = g * W
            u = E[t + 1, W + z0 : W + z0 + W].reshape(W * rows, cols)
            uh, ul = split(u)
            lap = dot(uh, CH[...]) + dot(ul, CH[...]) + dot(uh, CL[...])
            for j in range(W):
                z = z0 + j
                part = slice(j * rows, (j + 1) * rows)
                up = u[part]
                acc = lap[part] + (3.0 * COEFFS[0]) * up
                acc = acc + dot(yh, uh[part]) + dot(yh, ul[part]) + dot(yl, uh[part])
                for i in range(1, 5):
                    if z + i < depth:
                        acc = acc + COEFFS[i] * E[t + 1, W + z + i]
                    if z - i >= 0:
                        acc = acc + COEFFS[i] * E[t + 1, W + z - i]
                inject = dot(PR[z], QH[t]) + dot(PR[z], QL[t])
                E[t + 2, W + z] = 2.0 * up - E[t, W + z] + cour[z] * acc + inject

    local(0)

    def decode():
        i = lax.broadcasted_iota(jnp.int32, (rows, rows * blocks), 0)
        j = lax.broadcasted_iota(jnp.int32, (rows, rows * blocks), 1)
        flat = SC[...].reshape(128, rows * blocks)
        high = flat.astype(BF16)
        rest = flat - high.astype(F32)
        pieces = (high,) + split(rest)
        for m in range(blocks):
            pick = jnp.where(j == blocks * i + m, 1.0, 0.0).astype(BF16)
            moved = jnp.zeros((rows, 128), F32)
            for piece in pieces:
                moved = moved + lax.dot_general(
                    pick, piece, (((1,), (1,)), ((), ())), preferred_element_type=F32
                )
            TS[m] = moved

        @pl.loop(0, depth)
        def _(z):
            for m in range(blocks):
                xs = slice(m * QBLOCK, (m + 1) * QBLOCK)
                scale = pltpu.roll(TS[m], lax.rem(128 - z, 128), 1)
                f = []
                for k in range(ITERS + 2):
                    code = jnp.bitwise_and(jnp.right_shift(words[k, z], 8 * m), 255) - 128
                    f.append(code.astype(F32) * scale[:, k * depth : k * depth + 1])
                for t in range(ITERS):
                    k = ITERS - t
                    diff = f[k + 1] - 2.0 * f[k] + f[k - 1]
                    if t == 0:
                        IM[z, :, xs] = E[1, W + z, :, xs] * diff
                    else:
                        D[t - 1, z, :, xs] = diff

    for d in range(1, nshot):
        misfit_copy(d).wait()
    total = MB[0]
    for d in range(1, nshot):
        total = total + MB[d]
    ST[...] = total
    SB[pl.ds(space, 1)] = total.reshape(1, 8, 128)

    @pl.loop(1, nspace)
    def _(d):
        total_copy(d).start()

    def fix(t, c):
        ys = pl.ds(c * ych, ych)

        @pl.when(has_low)
        def _():
            halo(t, c, True).wait_recv()
            for j in range(W):
                acc = COEFFS[j + 1] * E[t + 1, W - 1, ys, :]
                for i in range(j + 2, 5):
                    acc = acc + COEFFS[i] * E[t + 1, W + j - i, ys, :]
                E[t + 2, W + j, ys, :] += cour[j, ys, :] * acc

        @pl.when(has_high)
        def _():
            halo(t, c, False).wait_recv()
            for j in range(W):
                z = depth - 1 - j
                acc = COEFFS[j + 1] * E[t + 1, W + depth, ys, :]
                for i in range(j + 2, 5):
                    acc = acc + COEFFS[i] * E[t + 1, W + z + i, ys, :]
                E[t + 2, W + z, ys, :] += cour[z, ys, :] * acc

    @pl.loop(0, ITERS - 1)
    def _(t):
        for c in range(NC):
            fix(t, c)

            @pl.when(has_high)
            def _():
                halo(t + 1, c, True).start()

            @pl.when(has_low)
            def _():
                halo(t + 1, c, False).start()

            if c == 0:

                @pl.when(t == 0)
                def _():
                    decode()

        local(t + 1)

        @pl.loop(0, depth)
        def _(z):
            IM[z] = IM[z] + E[t + 2, W + z] * D[t, z]

    out_second = pltpu.make_async_copy(E.at[ITERS, pl.ds(W, depth)], second_h, local_sem.at[4])
    out_second.start()
    inner = depth - 2 * W
    out_inner = pltpu.make_async_copy(
        E.at[ITERS + 1, pl.ds(2 * W, inner)], first_h.at[pl.ds(W, inner)], local_sem.at[5]
    )
    out_inner.start()

    first_z = space * depth

    @pl.loop(0, depth)
    def _(z):
        dz = first_z + z - source_s[0]
        dy = lax.broadcasted_iota(jnp.int32, (rows, cols), 0) - source_s[1]
        dx = lax.broadcasted_iota(jnp.int32, (rows, cols), 1) - source_s[2]
        dist = (dz * dz + dy * dy + dx * dx).astype(F32)
        IM[z] = IM[z] * (1.0 - jnp.exp(dist * (-1.0 / (2.0 * MUTE * MUTE))))

    core = lax.rem(shot, 2)
    pair = shot // 2
    pairs = nshot // 2
    yq = rows // nshot

    def quarter(index):
        return pl.ds(pl.multiple_of(index * yq, yq), yq)

    def copy_a(h):
        return pltpu.make_async_remote_copy(
            src_ref=IM.at[:, quarter(2 * h + 1 - core), :],
            dst_ref=RA.at[h],
            send_sem=a_send.at[h],
            recv_sem=a_recv.at[h],
            device_id={"shot": shot + 1 - 2 * core},
            device_id_type=MESH,
        )

    def copy_b(d):
        target = lax.rem(pair + d, pairs)
        return pltpu.make_async_remote_copy(
            src_ref=S.at[target],
            dst_ref=RB.at[d - 1],
            send_sem=b_send.at[d - 1],
            recv_sem=b_recv.at[d - 1],
            device_id={"shot": 2 * target + core},
            device_id_type=MESH,
        )

    for h in range(pairs):
        copy_a(h).start()
    for h in range(pairs):
        copy_a(h).wait()
        S[h] = IM[:, quarter(2 * h + core), :] + RA[h]
    for d in range(1, pairs):
        copy_b(d).start()

    for c in range(NC):
        fix(ITERS - 1, c)
    out_low = pltpu.make_async_copy(
        E.at[ITERS + 1, pl.ds(W, W)], first_h.at[pl.ds(0, W)], local_sem.at[6]
    )
    out_high = pltpu.make_async_copy(
        E.at[ITERS + 1, pl.ds(depth, W)], first_h.at[pl.ds(depth - W, W)], local_sem.at[7]
    )
    out_low.start()
    out_high.start()

    total = S[pair]
    for d in range(1, pairs):
        copy_b(d).wait()
        total = total + RB[d - 1]
    grad[...] = total

    @pl.loop(1, nspace)
    def _(d):
        total_copy(d).wait()

    whole = SB[0]
    for d in range(1, nspace):
        whole = whole + SB[d]
    misfit[...] = whole

    for c in range(NC):

        @pl.when(has_high)
        def _():
            halo_first(c, True).wait_send()

        @pl.when(has_low)
        def _():
            halo_first(c, False).wait_send()

        @pl.loop(1, ITERS)
        def _(t):
            @pl.when(has_high)
            def _():
                halo(t, c, True).wait_send()

            @pl.when(has_low)
            def _():
                halo(t, c, False).wait_send()

    out_second.wait()
    out_inner.wait()
    out_low.wait()
    out_high.wait()


def finish(factor, grad, first, second, total, grad_o, first_o, second_o, misfit, GB, FB, sem_in, sem_out):
    parts = FB.shape[0] // 2
    planes = FB.shape[1]
    moves = []
    for n, (source, target) in enumerate(((first, first_o), (second, second_o))):
        for p in range(parts):
            at = pl.ds(p * planes, planes)
            moves.append((source.at[at], FB.at[n * parts + p], target.at[at]))
    moves.append((grad, GB, grad_o))
    into = [
        pltpu.make_async_copy(source, held, sem_in.at[n])
        for n, (source, held, target) in enumerate(moves)
    ]
    out = [
        pltpu.make_async_copy(held, target, sem_out.at[n])
        for n, (source, held, target) in enumerate(moves)
    ]
    for copy in into:
        copy.start()
    misfit[...] = total[0:1, 0:1] * factor
    for n in range(len(moves)):
        into[n].wait()
        out[n].start()
    for copy in out:
        copy.wait()


def body(
    nshot,
    nspace,
    adjoint_now,
    adjoint_later,
    courant,
    checkpoint_codes,
    scale_index,
    scale_table,
    receiver_cell,
    observed,
    source_cell,
):
    depth, rows, cols = courant.shape
    levels = checkpoint_codes.shape[1]
    nrec = receiver_cell.shape[1]
    blocks = cols // QBLOCK
    pairs = nshot // 2
    yq = rows // nshot
    vmem = pl.BlockSpec(memory_space=pltpu.VMEM)
    smem = pl.BlockSpec(memory_space=pltpu.SMEM)
    anyspace = pl.BlockSpec(memory_space=pl.ANY)
    dma = pltpu.SemaphoreType.DMA
    field = jax.ShapeDtypeStruct((depth, rows, cols), F32)
    gradient, first, second, total = pl.pallas_call(
        functools.partial(kernel, nshot, nspace),
        out_shape=(
            jax.ShapeDtypeStruct((depth, yq, cols), F32),
            field,
            field,
            jax.ShapeDtypeStruct((8, 128), F32),
        ),
        in_specs=[smem] * 4 + [anyspace] * 4 + [vmem] * 2,
        out_specs=(vmem, anyspace, anyspace, vmem),
        scratch_shapes=[
            pltpu.VMEM((ITERS + 2, depth + 2 * W, rows, cols), F32),
            pltpu.VMEM((ITERS - 1, depth, rows, cols), F32),
            pltpu.VMEM((depth, rows, cols), F32),
            pltpu.VMEM((levels, depth, rows, QBLOCK), jnp.int32),
            pltpu.VMEM((128 // depth, depth, rows * blocks), F32),
            pltpu.VMEM((blocks, rows, 128), F32),
            pltpu.VMEM((nrec, 128), jnp.int32),
            pltpu.VMEM((ITERS, nrec, 128), F32),
            pltpu.VMEM((depth, rows, cols), F32),
            pltpu.VMEM((pairs, depth, yq, cols), F32),
            pltpu.VMEM((pairs, depth, yq, cols), F32),
            pltpu.VMEM((max(pairs - 1, 1), depth, yq, cols), F32),
            pltpu.VMEM((depth, rows, nrec), BF16),
            pltpu.VMEM((ITERS, nrec, cols), BF16),
            pltpu.VMEM((ITERS, nrec, cols), BF16),
            pltpu.VMEM((cols, cols), BF16),
            pltpu.VMEM((cols, cols), BF16),
            pltpu.VMEM((ITERS, nrec, QBLOCK), jnp.int32),
            pltpu.VMEM((ITERS, nrec, rows * blocks), F32),
            pltpu.VMEM((nshot, 8, 128), F32),
            pltpu.VMEM((nspace, 8, 128), F32),
            pltpu.VMEM((8, 128), F32),
            pltpu.VMEM((8, 128), F32),
            dma((2, ITERS, NC)),
            dma((2, ITERS, NC)),
            dma((pairs,)),
            dma((pairs,)),
            dma((max(pairs - 1, 1),)),
            dma((max(pairs - 1, 1),)),
            dma((nshot - 1,)),
            dma((nshot - 1,)),
            dma((nspace - 1,)),
            dma((nspace - 1,)),
            dma((8,)),
        ],
        compiler_params=pltpu.CompilerParams(
            collective_id=0, has_side_effects=True, vmem_limit_bytes=66000000
        ),
    )(
        receiver_cell[0],
        source_cell[0],
        scale_table,
        observed[0],
        adjoint_now[0],
        adjoint_later[0],
        courant,
        checkpoint_codes[0],
        scale_index[0],
        receiver_cell,
    )
    count = nshot * ITERS * nrec * nspace
    parts = depth // W
    gradient, first, second, misfit = pl.pallas_call(
        functools.partial(finish, 0.5 / count),
        out_shape=(jax.ShapeDtypeStruct(gradient.shape, F32), field, field, jax.ShapeDtypeStruct((1, 1), F32)),
        in_specs=[anyspace] * 3 + [vmem],
        out_specs=(anyspace, anyspace, anyspace, vmem),
        scratch_shapes=[
            pltpu.VMEM((depth, yq, cols), F32),
            pltpu.VMEM((2 * parts, W, rows, cols), F32),
            dma((2 * parts + 1,)),
            dma((2 * parts + 1,)),
        ],
    )(gradient, first, second, total)
    return (gradient, first[None], second[None], misfit.reshape(()))


def solution(mesh):
    placed = (
        P("shot", "space", None, None),
        P("shot", "space", None, None),
        P("space", None, None),
        P("shot", None, "space", None, None),
        P("shot", None, "space", None),
        P(),
        P("shot", "space"),
        P("shot", None, "space"),
        P("shot", None),
    )
    return jax.shard_map(
        functools.partial(body, mesh.shape["shot"], mesh.shape["space"]),
        mesh=mesh,
        in_specs=placed,
        out_specs=(
            P("space", "shot", None),
            P("shot", "space", None, None),
            P("shot", "space", None, None),
            P(),
        ),
        check_vma=False,
    )
```
